32 devices in a mesh: section: 4 (over y, core), seq: 8 (over z, x).
Axes of the slice: x: 2, y: 2, z: 4, core: 2. Of those that a mesh axis runs over, the one named last changes fastest.
Arguments:
- acts: bfloat16 [4, 1024, 2560], P('section', 'seq'), may hold values from -6 to 6
- feed: bfloat16 [1, 1024, 2560], P(None, 'seq'), may hold values from -6 to 6
- norm_gain: float32 [4, 2560], P('section'), may hold values from 0.5 to 1.5
- conv_weight: bfloat16 [4, 4, 2560], P('section'), may hold values from -3 to 3
- conv_bias: float32 [4, 2560], P('section'), may hold values from -3 to 3
- x_proj: bfloat16 [4, 2560, 192], P('section'), may hold values from -0.125 to 0.125
- dt_proj: bfloat16 [4, 160, 2560], P('section'), may hold values from -0.5 to 0.5
- dt_bias: float32 [4, 2560], P('section'), may hold values from -3 to 0.5
- a_rate: float32 [4, 16, 2560], P('section'), may hold values from 1.953125e-05 to 0.5
- skip: float32 [4, 2560], P('section'), may hold values from 0.5 to 1.5
Outputs:
- layer_outputs: bfloat16 [2, 4, 1024, 2560], P(None, 'section', 'seq')
The draws below stay inside these ranges and needn't reach their ends.
All inputs are finite; a program needn't handle non-finite values.
Results may differ from the reference program's by a relative error of at most 0.0062.
Values may be sent and summed in bfloat16 or wider, within the bound.
A program may use at most 64 MiB of HBM per device.

```python
import math
import jax
import jax.numpy as jnp
from jax import lax

INNER = 2560
STATE = 16
RANK = 160
KERNEL = 4
TICKS = 2
SECTIONS = 4
TOKENS = 1024


def block_levels(stream_key, extent, split, low, top_value):
    level, own = 1.0, jax.random.fold_in(stream_key, 6)
    for dim, parts in split:
        heights = jnp.exp(jax.random.uniform(jax.random.fold_in(own, dim), (parts,), jnp.float32, low / len(split), top_value / len(split)))
        level = level * jnp.repeat(heights, extent[dim] // parts).reshape([-1 if axis == dim else 1 for axis in range(len(extent))])
    return level


def bell_draw(key, extent, scale, bound, shards=(), held_as=jnp.bfloat16):
    level = block_levels(key, extent, shards, -0.22, 0.18) if shards else 1.0
    drawn = jax.random.normal(key, extent, jnp.float32) * scale * level
    return jnp.minimum(jnp.maximum(drawn, -bound), bound).astype(held_as)


def setup_inputs(seed: int = 0) -> dict:
    keys = jax.random.split(jax.random.key(seed), 11)
    acts = bell_draw(keys[0], (SECTIONS, TOKENS, INNER), 1.0, 6.0, ((0, 4), (1, 8)))
    feed = bell_draw(keys[1], (TICKS - 1, TOKENS, INNER), 1.0, 6.0, ((1, 8),))
    norm_gain = jnp.clip(1.0 + 0.1 * jax.random.normal(keys[2], (SECTIONS, INNER), jnp.float32), 0.5, 1.5)
    conv_weight = bell_draw(keys[3], (SECTIONS, KERNEL, INNER), KERNEL ** -0.5, 3.0, ((0, 4),))
    conv_bias = bell_draw(keys[4], (SECTIONS, INNER), 0.5, 3.0, ((0, 4),), jnp.float32)
    x_proj = bell_draw(keys[5], (SECTIONS, INNER, RANK + 2 * STATE), INNER ** -0.5, 0.125, ((0, 4),))
    dt_proj = bell_draw(keys[6], (SECTIONS, RANK, INNER), RANK ** -0.5, 0.5, ((0, 4),))
    dt_bias = jnp.clip(-3.0 + 3.5 * jax.random.uniform(keys[7], (SECTIONS, INNER), jnp.float32) ** block_levels(keys[7], (SECTIONS, INNER), ((0, 4),), -0.2, 0.2), -3.0, 0.5)
    a_rate = jnp.clip(jnp.exp(math.log(0.5) - 10.150348 * jax.random.uniform(keys[8], (SECTIONS, STATE, INNER), jnp.float32) ** block_levels(keys[8], (SECTIONS, STATE, INNER), ((0, 4),), -0.2, 0.2)), 1.9531249563442543e-05, 0.5)
    skip = jnp.clip(0.5 + 1.0 * jax.random.uniform(keys[9], (SECTIONS, INNER), jnp.float32) ** block_levels(keys[9], (SECTIONS, INNER), ((0, 4),), -0.2, 0.2), 0.5, 1.5)
    return dict(acts=acts, feed=feed, norm_gain=norm_gain, conv_weight=conv_weight, conv_bias=conv_bias, x_proj=x_proj, dt_proj=dt_proj, dt_bias=dt_bias, a_rate=a_rate, skip=skip)


def layer(pack):
    current, gain, conv_w, conv_b, x_w, dt_w, dt_b, rates, skip_w = pack
    values = current.astype(jnp.float32)
    normed = values * lax.rsqrt(lax.optimization_barrier(jnp.mean(values * values, axis=-1, keepdims=True)) + 1e-05) * gain
    padded = jnp.concatenate([jnp.zeros((KERNEL - 1, INNER), jnp.float32), normed], 0)
    conv = jnp.zeros((TOKENS, INNER), jnp.float32) + conv_b
    for shift_k in range(KERNEL):
        conv = conv + conv_w[shift_k].astype(jnp.float32) * padded[shift_k:shift_k + TOKENS]
    mixed = jax.nn.silu(conv).astype(jnp.bfloat16)
    proj = jnp.dot(mixed, x_w, preferred_element_type=jnp.float32)
    dt_low = proj[:, :RANK].astype(jnp.bfloat16)
    bmat = proj[:, RANK:RANK + STATE]
    cmat = proj[:, RANK + STATE:]
    steps = jax.nn.softplus(jnp.dot(dt_low, dt_w, preferred_element_type=jnp.float32) + dt_b)
    inputs = mixed.astype(jnp.float32)
    drive = steps * inputs

    def advance(state, row):
        step_row, drive_row, b_row, c_row = row
        state = jnp.exp(-step_row[None, :] * rates) * state + b_row[:, None] * drive_row[None, :]
        return (state, lax.optimization_barrier(jnp.sum(c_row[:, None] * state, axis=0)))
    start = jnp.zeros((STATE, INNER), jnp.float32)
    _, outputs = lax.scan(advance, start, (steps, drive, bmat, cmat))
    return (outputs + skip_w * inputs).astype(jnp.bfloat16)

def reference(acts, feed, norm_gain, conv_weight, conv_bias, x_proj, dt_proj, dt_bias, a_rate, skip):
    weights = (norm_gain, conv_weight, conv_bias, x_proj, dt_proj, dt_bias, a_rate, skip)
    current = acts
    results = []
    for tick in range(TICKS):
        result = lax.map(layer, (current,) + weights)
        results.append(result)
        if tick + 1 < TICKS:
            current = jnp.concatenate([feed[tick][None], result[:-1]], 0)
    return jnp.stack(results, 0)
```

```python
import functools
import math

import jax
import jax.numpy as jnp
from jax import lax
from jax.experimental import pallas as pl
from jax.experimental.pallas import tpu as pltpu
from jax.sharding import PartitionSpec as P

STATE = 16
RANK = 160
KERNEL = 4
TICKS = 2
GROUP = 16
PAD = 8
LOG2E = math.log2(math.e)


def prefix(shard, axis, combine, identity):
    size, position = (lax.axis_size(axis), lax.axis_index(axis))
    everything = jax.tree.map(lambda part: lax.all_gather(part, axis), shard)
    start = jax.tree.map(
        lambda part, zero: jnp.broadcast_to(jnp.asarray(zero, part.dtype), part.shape),
        shard,
        identity,
    )

    def step(k, before):
        reached = k < position
        new = combine(before, jax.tree.map(lambda part: part[k], everything))
        return jax.tree.map(lambda a, b: jnp.where(reached, a, b), new, before)

    return lax.fori_loop(0, size, step, start)


def passed_along(value, axis, steps):
    count = lax.axis_size(axis)
    initial, last = (max(0, -steps), min(count, count - steps))
    return lax.ppermute(value, axis, [(source, source + steps) for source in range(initial, last)])


def pass_carries(totals, ends, rates):

    def link(earlier, later):
        return (earlier[0] + later[0], jnp.exp(-rates * later[0]) * earlier[1] + later[1])

    empty = (jnp.zeros_like(totals), jnp.zeros_like(ends))
    _, incoming = prefix((totals, ends), "seq", link, empty)
    return incoming


def tile_of(width):
    return next(tile for tile in (512, 256, 128, width) if width % tile == 0)


def block_diagonal(cmat):
    rows = cmat.shape[0]
    wide = GROUP * STATE
    pick = lax.broadcasted_iota(jnp.int32, (STATE, wide), 0) == lax.broadcasted_iota(jnp.int32, (STATE, wide), 1) % STATE
    spread = jnp.dot(cmat.astype(jnp.bfloat16), pick.astype(jnp.bfloat16), preferred_element_type=jnp.float32)
    own = lax.broadcasted_iota(jnp.int32, (rows, wide), 0) % GROUP == lax.broadcasted_iota(jnp.int32, (rows, wide), 1) // STATE
    return jnp.where(own, spread, 0.0).astype(jnp.bfloat16)


def scan_kernel(cur, before, gain, conv_w, conv_b, x_w, dt_w, dt_b, rates, skip_w,
                out, ends, summed, cblk, normed, mixed, steps, drive, bwide, hist):
    rows, width = cur.shape
    tile = tile_of(width)
    tiles = width // tile
    groups = rows // GROUP

    def norm(rows_bf):
        values = rows_bf.astype(jnp.float32)
        return values * lax.rsqrt(jnp.mean(values * values, axis=-1, keepdims=True) + 1e-05) * gain[...]

    normed[pl.ds(0, PAD), :] = norm(before[...])

    @pl.loop(0, rows // 16)
    def _(g):
        at = pl.multiple_of(g * 16, 16)
        normed[pl.ds(pl.multiple_of(at + PAD, PAD), 16), :] = norm(cur[pl.ds(at, 16), :])

    @pl.loop(0, tiles)
    def _(c):
        cols = pl.ds(pl.multiple_of(c * tile, tile), tile)
        conv = jnp.broadcast_to(conv_b[:, cols], (rows, tile))
        for k in range(KERNEL):
            conv = conv + conv_w[k:k + 1, cols].astype(jnp.float32) * normed[PAD - KERNEL + 1 + k:PAD - KERNEL + 1 + k + rows, cols]
        mixed[:, cols] = (conv * jax.nn.sigmoid(conv)).astype(jnp.bfloat16)

    proj = jnp.dot(mixed[...], x_w[...], preferred_element_type=jnp.float32)
    dt_low = proj[:, :RANK].astype(jnp.bfloat16)
    bmat = proj[:, RANK:RANK + STATE]
    cmat = proj[:, RANK + STATE:]
    cblk[...] = block_diagonal(cmat)
    bcols = bmat.T
    for t in range(rows):
        bwide[t] = jnp.broadcast_to(bcols[:, t:t + 1], (STATE, 128))
    lower = (lax.broadcasted_iota(jnp.int32, (rows, rows), 0) >= lax.broadcasted_iota(jnp.int32, (rows, rows), 1)).astype(jnp.bfloat16)

    @pl.loop(0, tiles)
    def _(c):
        cols = pl.ds(pl.multiple_of(c * tile, tile), tile)
        raw = jnp.dot(dt_low, dt_w[:, cols], preferred_element_type=jnp.float32) + dt_b[:, cols]
        step = jnp.maximum(raw, 0.0) + jnp.log1p(jnp.exp(-jnp.abs(raw)))
        steps[:, cols] = step
        drive[:, cols] = step * mixed[:, cols].astype(jnp.float32)
        high = step.astype(jnp.bfloat16)
        low = (step - high.astype(jnp.float32)).astype(jnp.bfloat16)
        summed[:, cols] = jnp.dot(lower, high, preferred_element_type=jnp.float32) + jnp.dot(lower, low, preferred_element_type=jnp.float32)

    @pl.loop(0, tiles)
    def _(c):
        cols = pl.ds(pl.multiple_of(c * tile, tile), tile)
        decay = rates[:, cols] * (-LOG2E)

        def emit(g):
            span = pl.ds(pl.multiple_of(g * GROUP, GROUP), GROUP)
            past = hist[pl.ds(pl.multiple_of(g * GROUP * STATE, GROUP * STATE), GROUP * STATE), :]
            local = jnp.dot(cblk[span, :], past, preferred_element_type=jnp.float32)
            out[span, cols] = local + skip_w[:, cols] * mixed[span, cols].astype(jnp.float32)

        def group(g, state):
            emit(jnp.maximum(g - 1, 0))
            at = pl.multiple_of(g * GROUP, GROUP)
            step_blk = steps[pl.ds(at, GROUP), cols]
            drive_blk = drive[pl.ds(at, GROUP), cols]
            for i in range(GROUP):
                b_row = jnp.concatenate([bwide[at + i]] * (tile // 128), axis=1)
                state = jnp.exp2(step_blk[i:i + 1] * decay) * state + b_row * drive_blk[i:i + 1]
                hist[pl.ds(pl.multiple_of((at + i) * STATE, STATE), STATE), :] = state.astype(jnp.bfloat16)
            return state

        ends[:, cols] = lax.fori_loop(0, groups, group, jnp.zeros((STATE, tile), jnp.float32))
        emit(groups - 1)


def fix_kernel(local, summed, cblk, incoming, rates, out, hist):
    rows, width = local.shape
    tile = tile_of(width)
    groups = rows // GROUP

    @pl.loop(0, width // tile)
    def _(c):
        cols = pl.ds(pl.multiple_of(c * tile, tile), tile)
        decay = rates[:, cols] * (-LOG2E)
        start = incoming[:, cols]

        def emit(g):
            span = pl.ds(pl.multiple_of(g * GROUP, GROUP), GROUP)
            past = hist[pl.ds(pl.multiple_of(g * GROUP * STATE, GROUP * STATE), GROUP * STATE), :]
            fixed = jnp.dot(cblk[span, :], past, preferred_element_type=jnp.float32)
            out[span, cols] = (local[span, cols] + fixed).astype(out.dtype)

        @pl.loop(0, groups)
        def _(g):
            emit(jnp.maximum(g - 1, 0))
            at = pl.multiple_of(g * GROUP, GROUP)
            sum_blk = summed[pl.ds(at, GROUP), cols]
            for i in range(GROUP):
                moved = jnp.exp2(sum_blk[i:i + 1] * decay) * start
                hist[pl.ds(pl.multiple_of((at + i) * STATE, STATE), STATE), :] = moved.astype(jnp.bfloat16)

        emit(groups - 1)


VMEM = pl.BlockSpec(memory_space=pltpu.VMEM)


def layer(current, before, gain, conv_w, conv_b, x_w, dt_w, dt_b, rates, skip_w):
    rows, width = current.shape
    tile = tile_of(width)
    f32, bf16 = jnp.float32, jnp.bfloat16
    local, ends, summed, cblk = pl.pallas_call(
        scan_kernel,
        out_shape=(
            jax.ShapeDtypeStruct((rows, width), f32),
            jax.ShapeDtypeStruct((STATE, width), f32),
            jax.ShapeDtypeStruct((rows, width), f32),
            jax.ShapeDtypeStruct((rows, GROUP * STATE), bf16),
        ),
        in_specs=[VMEM] * 10,
        out_specs=(VMEM,) * 4,
        scratch_shapes=[
            pltpu.VMEM((rows + PAD, width), f32),
            pltpu.VMEM((rows, width), bf16),
            pltpu.VMEM((rows, width), f32),
            pltpu.VMEM((rows, width), f32),
            pltpu.VMEM((rows, STATE, 128), f32),
            pltpu.VMEM((rows * STATE, tile), bf16),
        ],
        compiler_params=pltpu.CompilerParams(vmem_limit_bytes=40 << 20),
        name="local_scan",
    )(current, before, gain, conv_w, conv_b, x_w, dt_w, dt_b, rates, skip_w)
    incoming = pass_carries(summed[-1:], ends, rates)
    return pl.pallas_call(
        fix_kernel,
        out_shape=jax.ShapeDtypeStruct((rows, width), bf16),
        in_specs=[VMEM] * 5,
        out_specs=VMEM,
        scratch_shapes=[pltpu.VMEM((rows * STATE, tile), bf16)],
        compiler_params=pltpu.CompilerParams(vmem_limit_bytes=40 << 20),
        name="carry_fix",
    )(local, summed, cblk, incoming, rates)


def local(acts, feed, norm_gain, conv_weight, conv_bias, x_proj, dt_proj, dt_bias, a_rate, skip):
    section_zero = lax.axis_index("section") == 0
    seq_zero = lax.axis_index("seq") == 0
    weights = (norm_gain, conv_weight[0], conv_bias, x_proj[0], dt_proj[0], dt_bias, a_rate[0], skip)
    current = acts[0]
    prev_now, prev_feeds = passed_along((acts[0][-PAD:], feed[:, -PAD:, :]), "seq", 1)
    results = []
    for tick in range(TICKS):
        result = layer(current, prev_now, *weights)
        results.append(result)
        if tick + 1 < TICKS:
            received = passed_along(result, "section", 1)
            current = jnp.where(section_zero, feed[tick], received)
            diagonal = passed_along(result[-PAD:], ("section", "seq"), lax.axis_size("seq") + 1)
            diagonal = jnp.where(seq_zero, jnp.zeros_like(diagonal), diagonal)
            prev_now = jnp.where(section_zero, prev_feeds[tick], diagonal)
    return jnp.stack(results, 0)[:, None]


def solution(mesh):
    return jax.shard_map(
        local,
        mesh=mesh,
        in_specs=(
            P("section", "seq", None),
            P(None, "seq", None),
            P("section", None),
            P("section", None, None),
            P("section", None),
            P("section", None, None),
            P("section", None, None),
            P("section", None),
            P("section", None, None),
            P("section", None),
        ),
        out_specs=P(None, "section", "seq", None),
        check_vma=False,
    )
```

```python
import functools
import math

import jax
import jax.numpy as jnp
from jax import lax
from jax.experimental import pallas as pl
from jax.experimental.pallas import tpu as pltpu
from jax.sharding import PartitionSpec as P

STATE = 16
RANK = 160
KERNEL = 4
TICKS = 2
GROUP = 16
PAD = 8
LOG2E = math.log2(math.e)
MESH = pl.DeviceIdType.MESH
VMEM = pl.BlockSpec(memory_space=pltpu.VMEM)


def prefix(shard, axis, combine, identity):
    size, position = (lax.axis_size(axis), lax.axis_index(axis))
    everything = jax.tree.map(lambda part: lax.all_gather(part, axis), shard)
    start = jax.tree.map(
        lambda part, zero: jnp.broadcast_to(jnp.asarray(zero, part.dtype), part.shape),
        shard,
        identity,
    )

    def step(k, before):
        reached = k < position
        new = combine(before, jax.tree.map(lambda part: part[k], everything))
        return jax.tree.map(lambda a, b: jnp.where(reached, a, b), new, before)

    return lax.fori_loop(0, size, step, start)


def passed_along(value, axis, steps):
    count = lax.axis_size(axis)
    initial, last = (max(0, -steps), min(count, count - steps))
    return lax.ppermute(value, axis, [(source, source + steps) for source in range(initial, last)])


def pass_carries(totals, ends, rates):

    def link(earlier, later):
        return (earlier[0] + later[0], jnp.exp(-rates * later[0]) * earlier[1] + later[1])

    empty = (jnp.zeros_like(totals), jnp.zeros_like(ends))
    _, incoming = prefix((totals, ends), "seq", link, empty)
    return incoming


def relay_kernel(ends, totals, rates, incoming, pend, ptot, hin, hout, pairs, decays,
                 pend_send, pend_recv, tot_send, tot_recv, hin_recv, odd_send, even_send, *, size):
    me = lax.axis_index("seq")
    odd = lax.rem(me, 2) == 1
    chunks, _, tile = pend.shape
    later = jnp.logical_and(odd, me + 2 < size)
    earlier = me > 1
    barrier = pltpu.get_barrier_semaphore()

    def greet(where):
        pl.semaphore_signal(barrier, inc=1, device_id={"seq": where}, device_id_type=MESH)

    def cols(j):
        return pl.ds(j * tile, tile)

    def to_pair(j):
        return pltpu.make_async_remote_copy(ends.at[:, cols(j)], pend.at[j], pend_send.at[j], pend_recv.at[j],
                                            device_id={"seq": me + 1}, device_id_type=MESH)

    def to_pair_totals():
        return pltpu.make_async_remote_copy(totals, ptot, tot_send, tot_recv,
                                            device_id={"seq": me + 1}, device_id_type=MESH)

    def to_odd(j):
        return pltpu.make_async_remote_copy(hout.at[j], hin.at[j], odd_send.at[j], hin_recv.at[j],
                                            device_id={"seq": me + 2}, device_id_type=MESH)

    def to_even(j):
        return pltpu.make_async_remote_copy(hout.at[j], hin.at[j], even_send.at[j], hin_recv.at[j],
                                            device_id={"seq": me + 1}, device_id_type=MESH)

    @pl.when(me > 0)
    def _():
        greet(me - 1)

    @pl.when(jnp.logical_and(odd, earlier))
    def _():
        greet(me - 2)

    @pl.when(jnp.logical_not(odd))
    def _():
        pl.semaphore_wait(barrier, 1)
        to_pair_totals().start()
        for j in range(chunks):
            to_pair(j).start()

    @pl.when(later)
    def _():
        pl.semaphore_wait(barrier, 2)

    @pl.when(odd)
    def _():
        to_pair_totals().wait_recv()
        for j in range(chunks):
            at = cols(j)
            scale = rates[:, at] * (-LOG2E)
            decays[j] = jnp.exp2(scale * (ptot[:, at] + totals[:, at]))
            to_pair(j).wait_recv()
            pairs[j] = jnp.exp2(scale * totals[:, at]) * pend[j] + ends[:, at]

    @pl.when(jnp.logical_not(earlier))
    def _():
        hin[...] = jnp.zeros_like(hin)

    for j in range(chunks):
        @pl.when(earlier)
        def _():
            to_odd(j).wait_recv()

        @pl.when(later)
        def _():
            hout[j] = decays[j] * hin[j] + pairs[j]
            to_odd(j).start()
            to_even(j).start()

    @pl.when(odd)
    def _():
        for j in range(chunks):
            at = cols(j)
            incoming[:, at] = jnp.exp2(rates[:, at] * (-LOG2E) * ptot[:, at]) * hin[j] + pend[j]

    @pl.when(jnp.logical_not(odd))
    def _():
        for j in range(chunks):
            incoming[:, cols(j)] = hin[j]
        to_pair_totals().wait_send()
        for j in range(chunks):
            to_pair(j).wait_send()

    @pl.when(later)
    def _():
        for j in range(chunks):
            to_odd(j).wait_send()
            to_even(j).wait_send()


def relay_carries(totals, ends, rates):
    size = lax.axis_size("seq")
    if size % 2:
        return pass_carries(totals, ends, rates)
    width = ends.shape[1]
    tile = tile_of(width)
    chunks = width // tile
    f32 = jnp.float32
    slots = pltpu.VMEM((chunks, STATE, tile), f32)
    each = pltpu.SemaphoreType.DMA((chunks,))
    return pl.pallas_call(
        functools.partial(relay_kernel, size=size),
        out_shape=jax.ShapeDtypeStruct((STATE, width), f32),
        in_specs=[VMEM] * 3,
        out_specs=VMEM,
        scratch_shapes=[slots, pltpu.VMEM((1, width), f32), slots, slots, slots, slots,
                        each, each, pltpu.SemaphoreType.DMA, pltpu.SemaphoreType.DMA, each, each, each],
        compiler_params=pltpu.CompilerParams(collective_id=0, has_side_effects=True, vmem_limit_bytes=16 << 20),
        name="carry_relay",
    )(ends, totals, rates)


def tile_of(width):
    return next(tile for tile in (512, 256, 128, width) if width % tile == 0)


def block_diagonal(cmat):
    rows = cmat.shape[0]
    wide = GROUP * STATE
    pick = lax.broadcasted_iota(jnp.int32, (STATE, wide), 0) == lax.broadcasted_iota(jnp.int32, (STATE, wide), 1) % STATE
    spread = jnp.dot(cmat.astype(jnp.bfloat16), pick.astype(jnp.bfloat16), preferred_element_type=jnp.float32)
    own = lax.broadcasted_iota(jnp.int32, (rows, wide), 0) % GROUP == lax.broadcasted_iota(jnp.int32, (rows, wide), 1) // STATE
    return jnp.where(own, spread, 0.0).astype(jnp.bfloat16)


def scan_kernel(cur, before, gain, conv_w, conv_b, x_w, dt_w, dt_b, rates, skip_w,
                out, ends, summed, cblk, normed, mixed, steps, drive, bwide, hist):
    rows, width = cur.shape
    tile = tile_of(width)
    tiles = width // tile
    groups = rows // GROUP

    def norm(rows_bf):
        values = rows_bf.astype(jnp.float32)
        return values * lax.rsqrt(jnp.mean(values * values, axis=-1, keepdims=True) + 1e-05) * gain[...]

    normed[pl.ds(0, PAD), :] = norm(before[...])

    @pl.loop(0, rows // 16)
    def _(g):
        at = pl.multiple_of(g * 16, 16)
        normed[pl.ds(pl.multiple_of(at + PAD, PAD), 16), :] = norm(cur[pl.ds(at, 16), :])

    @pl.loop(0, tiles)
    def _(c):
        cols = pl.ds(pl.multiple_of(c * tile, tile), tile)
        conv = jnp.broadcast_to(conv_b[:, cols], (rows, tile))
        for k in range(KERNEL):
            conv = conv + conv_w[k:k + 1, cols].astype(jnp.float32) * normed[PAD - KERNEL + 1 + k:PAD - KERNEL + 1 + k + rows, cols]
        mixed[:, cols] = (conv * jax.nn.sigmoid(conv)).astype(jnp.bfloat16)

    proj = jnp.dot(mixed[...], x_w[...], preferred_element_type=jnp.float32)
    dt_low = proj[:, :RANK].astype(jnp.bfloat16)
    bmat = proj[:, RANK:RANK + STATE]
    cmat = proj[:, RANK + STATE:]
    cblk[...] = block_diagonal(cmat)
    bcols = bmat.T
    for t in range(rows):
        bwide[t] = jnp.broadcast_to(bcols[:, t:t + 1], (STATE, 128))
    lower = (lax.broadcasted_iota(jnp.int32, (rows, rows), 0) >= lax.broadcasted_iota(jnp.int32, (rows, rows), 1)).astype(jnp.bfloat16)

    @pl.loop(0, tiles)
    def _(c):
        cols = pl.ds(pl.multiple_of(c * tile, tile), tile)
        raw = jnp.dot(dt_low, dt_w[:, cols], preferred_element_type=jnp.float32) + dt_b[:, cols]
        step = jnp.maximum(raw, 0.0) + jnp.log1p(jnp.exp(-jnp.abs(raw)))
        steps[:, cols] = step
        drive[:, cols] = step * mixed[:, cols].astype(jnp.float32)
        high = step.astype(jnp.bfloat16)
        low = (step - high.astype(jnp.float32)).astype(jnp.bfloat16)
        summed[:, cols] = jnp.dot(lower, high, preferred_element_type=jnp.float32) + jnp.dot(lower, low, preferred_element_type=jnp.float32)

    @pl.loop(0, tiles)
    def _(c):
        cols = pl.ds(pl.multiple_of(c * tile, tile), tile)
        decay = rates[:, cols] * (-LOG2E)

        def emit(g):
            span = pl.ds(pl.multiple_of(g * GROUP, GROUP), GROUP)
            past = hist[pl.ds(pl.multiple_of(g * GROUP * STATE, GROUP * STATE), GROUP * STATE), :]
            local = jnp.dot(cblk[span, :], past, preferred_element_type=jnp.float32)
            out[span, cols] = local + skip_w[:, cols] * mixed[span, cols].astype(jnp.float32)

        def group(g, state):
            emit(jnp.maximum(g - 1, 0))
            at = pl.multiple_of(g * GROUP, GROUP)
            step_blk = steps[pl.ds(at, GROUP), cols]
            drive_blk = drive[pl.ds(at, GROUP), cols]
            for i in range(GROUP):
                b_row = jnp.concatenate([bwide[at + i]] * (tile // 128), axis=1)
                state = jnp.exp2(step_blk[i:i + 1] * decay) * state + b_row * drive_blk[i:i + 1]
                hist[pl.ds(pl.multiple_of((at + i) * STATE, STATE), STATE), :] = state.astype(jnp.bfloat16)
            return state

        ends[:, cols] = lax.fori_loop(0, groups, group, jnp.zeros((STATE, tile), jnp.float32))
        emit(groups - 1)


def fix_kernel(local, summed, cblk, incoming, rates, out, hist):
    rows, width = local.shape
    tile = tile_of(width)
    groups = rows // GROUP

    @pl.loop(0, width // tile)
    def _(c):
        cols = pl.ds(pl.multiple_of(c * tile, tile), tile)
        decay = rates[:, cols] * (-LOG2E)
        start = incoming[:, cols]

        def emit(g):
            span = pl.ds(pl.multiple_of(g * GROUP, GROUP), GROUP)
            past = hist[pl.ds(pl.multiple_of(g * GROUP * STATE, GROUP * STATE), GROUP * STATE), :]
            fixed = jnp.dot(cblk[span, :], past, preferred_element_type=jnp.float32)
            out[span, cols] = (local[span, cols] + fixed).astype(out.dtype)

        @pl.loop(0, groups)
        def _(g):
            emit(jnp.maximum(g - 1, 0))
            at = pl.multiple_of(g * GROUP, GROUP)
            sum_blk = summed[pl.ds(at, GROUP), cols]
            for i in range(GROUP):
                moved = jnp.exp2(sum_blk[i:i + 1] * decay) * start
                hist[pl.ds(pl.multiple_of((at + i) * STATE, STATE), STATE), :] = moved.astype(jnp.bfloat16)

        emit(groups - 1)


def layer(current, before, gain, conv_w, conv_b, x_w, dt_w, dt_b, rates, skip_w):
    rows, width = current.shape
    tile = tile_of(width)
    f32, bf16 = jnp.float32, jnp.bfloat16
    local, ends, summed, cblk = pl.pallas_call(
        scan_kernel,
        out_shape=(
            jax.ShapeDtypeStruct((rows, width), f32),
            jax.ShapeDtypeStruct((STATE, width), f32),
            jax.ShapeDtypeStruct((rows, width), f32),
            jax.ShapeDtypeStruct((rows, GROUP * STATE), bf16),
        ),
        in_specs=[VMEM] * 10,
        out_specs=(VMEM,) * 4,
        scratch_shapes=[
            pltpu.VMEM((rows + PAD, width), f32),
            pltpu.VMEM((rows, width), bf16),
            pltpu.VMEM((rows, width), f32),
            pltpu.VMEM((rows, width), f32),
            pltpu.VMEM((rows, STATE, 128), f32),
            pltpu.VMEM((rows * STATE, tile), bf16),
        ],
        compiler_params=pltpu.CompilerParams(vmem_limit_bytes=40 << 20),
        name="local_scan",
    )(current, before, gain, conv_w, conv_b, x_w, dt_w, dt_b, rates, skip_w)
    incoming = relay_carries(summed[-1:], ends, rates)
    return pl.pallas_call(
        fix_kernel,
        out_shape=jax.ShapeDtypeStruct((rows, width), bf16),
        in_specs=[VMEM] * 5,
        out_specs=VMEM,
        scratch_shapes=[pltpu.VMEM((rows * STATE, tile), bf16)],
        compiler_params=pltpu.CompilerParams(vmem_limit_bytes=40 << 20),
        name="carry_fix",
    )(local, summed, cblk, incoming, rates)


def local(acts, feed, norm_gain, conv_weight, conv_bias, x_proj, dt_proj, dt_bias, a_rate, skip):
    section_zero = lax.axis_index("section") == 0
    seq_zero = lax.axis_index("seq") == 0
    weights = (norm_gain, conv_weight[0], conv_bias, x_proj[0], dt_proj[0], dt_bias, a_rate[0], skip)
    current = acts[0]
    prev_now, prev_feeds = passed_along((acts[0][-PAD:], feed[:, -PAD:, :]), "seq", 1)
    results = []
    for tick in range(TICKS):
        result = layer(current, prev_now, *weights)
        results.append(result)
        if tick + 1 < TICKS:
            received = passed_along(result, "section", 1)
            current = jnp.where(section_zero, feed[tick], received)
            diagonal = passed_along(result[-PAD:], ("section", "seq"), lax.axis_size("seq") + 1)
            diagonal = jnp.where(seq_zero, jnp.zeros_like(diagonal), diagonal)
            prev_now = jnp.where(section_zero, prev_feeds[tick], diagonal)
    return jnp.stack(results, 0)[:, None]


def solution(mesh):
    return jax.shard_map(
        local,
        mesh=mesh,
        in_specs=(
            P("section", "seq", None),
            P(None, "seq", None),
            P("section", None),
            P("section", None, None),
            P("section", None),
            P("section", None, None),
            P("section", None, None),
            P("section", None),
            P("section", None, None),
            P("section", None),
        ),
        out_specs=P(None, "section", "seq", None),
        check_vma=False,
    )
```

```python
import functools
import math

import jax
import jax.numpy as jnp
from jax import lax
from jax.experimental import pallas as pl
from jax.experimental.pallas import tpu as pltpu
from jax.sharding import PartitionSpec as P

STATE = 16
RANK = 160
KERNEL = 4
TICKS = 2
GROUP = 16
PAD = 8
LOG2E = math.log2(math.e)
MESH = pl.DeviceIdType.MESH
VMEM = pl.BlockSpec(memory_space=pltpu.VMEM)


def prefix(shard, axis, combine, identity):
    size, position = (lax.axis_size(axis), lax.axis_index(axis))
    everything = jax.tree.map(lambda part: lax.all_gather(part, axis), shard)
    start = jax.tree.map(
        lambda part, zero: jnp.broadcast_to(jnp.asarray(zero, part.dtype), part.shape),
        shard,
        identity,
    )

    def step(k, before):
        reached = k < position
        new = combine(before, jax.tree.map(lambda part: part[k], everything))
        return jax.tree.map(lambda a, b: jnp.where(reached, a, b), new, before)

    return lax.fori_loop(0, size, step, start)


def passed_along(value, axis, steps):
    count = lax.axis_size(axis)
    initial, last = (max(0, -steps), min(count, count - steps))
    return lax.ppermute(value, axis, [(source, source + steps) for source in range(initial, last)])


def pass_carries(totals, ends, rates):

    def link(earlier, later):
        return (earlier[0] + later[0], jnp.exp(-rates * later[0]) * earlier[1] + later[1])

    empty = (jnp.zeros_like(totals), jnp.zeros_like(ends))
    _, incoming = prefix((totals, ends), "seq", link, empty)
    return incoming


def relay_kernel(ends, totals, rates, incoming, pend, ptot, hin, hout, pairs, decays,
                 pend_send, pend_recv, tot_send, tot_recv, hin_recv, odd_send, even_send, *, size):
    me = lax.axis_index("seq")
    odd = lax.rem(me, 2) == 1
    chunks, _, tile = pend.shape
    later = jnp.logical_and(odd, me + 2 < size)
    earlier = me > 1
    barrier = pltpu.get_barrier_semaphore()

    def greet(where):
        pl.semaphore_signal(barrier, inc=1, device_id={"seq": where}, device_id_type=MESH)

    def cols(j):
        return pl.ds(j * tile, tile)

    def to_pair(j):
        return pltpu.make_async_remote_copy(ends.at[:, cols(j)], pend.at[j], pend_send.at[j], pend_recv.at[j],
                                            device_id={"seq": me + 1}, device_id_type=MESH)

    def to_pair_totals():
        return pltpu.make_async_remote_copy(totals, ptot, tot_send, tot_recv,
                                            device_id={"seq": me + 1}, device_id_type=MESH)

    def to_odd(j):
        return pltpu.make_async_remote_copy(hout.at[j], hin.at[j], odd_send.at[j], hin_recv.at[j],
                                            device_id={"seq": me + 2}, device_id_type=MESH)

    def to_even(j):
        return pltpu.make_async_remote_copy(hin.at[j], hin.at[j], even_send.at[j], hin_recv.at[j],
                                            device_id={"seq": me - 1}, device_id_type=MESH)

    onward = jnp.logical_and(odd, earlier)

    @pl.when(odd)
    def _():
        greet(me - 1)

    @pl.when(onward)
    def _():
        greet(me - 2)

    @pl.when(jnp.logical_and(jnp.logical_not(odd), earlier))
    def _():
        greet(me + 1)

    @pl.when(jnp.logical_not(odd))
    def _():
        pl.semaphore_wait(barrier, 1)
        to_pair_totals().start()
        for j in range(chunks):
            to_pair(j).start()

    @pl.when(jnp.logical_and(later, onward))
    def _():
        pl.semaphore_wait(barrier, 2)

    @pl.when(jnp.logical_and(odd, later != onward))
    def _():
        pl.semaphore_wait(barrier, 1)

    @pl.when(odd)
    def _():
        to_pair_totals().wait_recv()
        for j in range(chunks):
            at = cols(j)
            scale = rates[:, at] * (-LOG2E)
            decays[j] = jnp.exp2(scale * (ptot[:, at] + totals[:, at]))
            to_pair(j).wait_recv()
            pairs[j] = jnp.exp2(scale * totals[:, at]) * pend[j] + ends[:, at]

    @pl.when(jnp.logical_not(earlier))
    def _():
        hin[...] = jnp.zeros_like(hin)

    for j in range(chunks):
        @pl.when(earlier)
        def _():
            to_odd(j).wait_recv()

        @pl.when(later)
        def _():
            hout[j] = decays[j] * hin[j] + pairs[j]
            to_odd(j).start()

        @pl.when(onward)
        def _():
            to_even(j).start()

    @pl.when(odd)
    def _():
        for j in range(chunks):
            at = cols(j)
            incoming[:, at] = jnp.exp2(rates[:, at] * (-LOG2E) * ptot[:, at]) * hin[j] + pend[j]

    @pl.when(jnp.logical_not(odd))
    def _():
        for j in range(chunks):
            incoming[:, cols(j)] = hin[j]
        to_pair_totals().wait_send()
        for j in range(chunks):
            to_pair(j).wait_send()

    @pl.when(later)
    def _():
        for j in range(chunks):
            to_odd(j).wait_send()

    @pl.when(onward)
    def _():
        for j in range(chunks):
            to_even(j).wait_send()


def relay_carries(totals, ends, rates):
    size = lax.axis_size("seq")
    if size % 2:
        return pass_carries(totals, ends, rates)
    width = ends.shape[1]
    tile = tile_of(width)
    chunks = width // tile
    f32 = jnp.float32
    slots = pltpu.VMEM((chunks, STATE, tile), f32)
    each = pltpu.SemaphoreType.DMA((chunks,))
    return pl.pallas_call(
        functools.partial(relay_kernel, size=size),
        out_shape=jax.ShapeDtypeStruct((STATE, width), f32),
        in_specs=[VMEM] * 3,
        out_specs=VMEM,
        scratch_shapes=[slots, pltpu.VMEM((1, width), f32), slots, slots, slots, slots,
                        each, each, pltpu.SemaphoreType.DMA, pltpu.SemaphoreType.DMA, each, each, each],
        compiler_params=pltpu.CompilerParams(collective_id=0, has_side_effects=True, vmem_limit_bytes=16 << 20),
        name="carry_relay",
    )(ends, totals, rates)


def tile_of(width):
    return next(tile for tile in (512, 256, 128, width) if width % tile == 0)


def block_diagonal(cmat):
    rows = cmat.shape[0]
    wide = GROUP * STATE
    pick = lax.broadcasted_iota(jnp.int32, (STATE, wide), 0) == lax.broadcasted_iota(jnp.int32, (STATE, wide), 1) % STATE
    spread = jnp.dot(cmat.astype(jnp.bfloat16), pick.astype(jnp.bfloat16), preferred_element_type=jnp.float32)
    own = lax.broadcasted_iota(jnp.int32, (rows, wide), 0) % GROUP == lax.broadcasted_iota(jnp.int32, (rows, wide), 1) // STATE
    return jnp.where(own, spread, 0.0).astype(jnp.bfloat16)


def scan_kernel(cur, before, gain, conv_w, conv_b, x_w, dt_w, dt_b, rates, skip_w,
                out, ends, summed, cblk, normed, mixed, steps, drive, bwide, hist):
    rows, width = cur.shape
    tile = tile_of(width)
    tiles = width // tile
    groups = rows // GROUP

    def norm(rows_bf):
        values = rows_bf.astype(jnp.float32)
        return values * lax.rsqrt(jnp.mean(values * values, axis=-1, keepdims=True) + 1e-05) * gain[...]

    normed[pl.ds(0, PAD), :] = norm(before[...])

    @pl.loop(0, rows // 16)
    def _(g):
        at = pl.multiple_of(g * 16, 16)
        normed[pl.ds(pl.multiple_of(at + PAD, PAD), 16), :] = norm(cur[pl.ds(at, 16), :])

    @pl.loop(0, tiles)
    def _(c):
        cols = pl.ds(pl.multiple_of(c * tile, tile), tile)
        conv = jnp.broadcast_to(conv_b[:, cols], (rows, tile))
        for k in range(KERNEL):
            conv = conv + conv_w[k:k + 1, cols].astype(jnp.float32) * normed[PAD - KERNEL + 1 + k:PAD - KERNEL + 1 + k + rows, cols]
        mixed[:, cols] = (conv * jax.nn.sigmoid(conv)).astype(jnp.bfloat16)

    proj = jnp.dot(mixed[...], x_w[...], preferred_element_type=jnp.float32)
    dt_low = proj[:, :RANK].astype(jnp.bfloat16)
    bmat = proj[:, RANK:RANK + STATE]
    cmat = proj[:, RANK + STATE:]
    cblk[...] = block_diagonal(cmat)
    bcols = bmat.T
    for t in range(rows):
        bwide[t] = jnp.broadcast_to(bcols[:, t:t + 1], (STATE, 128))
    lower = (lax.broadcasted_iota(jnp.int32, (rows, rows), 0) >= lax.broadcasted_iota(jnp.int32, (rows, rows), 1)).astype(jnp.bfloat16)

    @pl.loop(0, tiles)
    def _(c):
        cols = pl.ds(pl.multiple_of(c * tile, tile), tile)
        raw = jnp.dot(dt_low, dt_w[:, cols], preferred_element_type=jnp.float32) + dt_b[:, cols]
        step = jnp.maximum(raw, 0.0) + jnp.log1p(jnp.exp(-jnp.abs(raw)))
        steps[:, cols] = step
        drive[:, cols] = step * mixed[:, cols].astype(jnp.float32)
        high = step.astype(jnp.bfloat16)
        low = (step - high.astype(jnp.float32)).astype(jnp.bfloat16)
        summed[:, cols] = jnp.dot(lower, high, preferred_element_type=jnp.float32) + jnp.dot(lower, low, preferred_element_type=jnp.float32)

    @pl.loop(0, tiles)
    def _(c):
        cols = pl.ds(pl.multiple_of(c * tile, tile), tile)
        decay = rates[:, cols] * (-LOG2E)

        def emit(g):
            span = pl.ds(pl.multiple_of(g * GROUP, GROUP), GROUP)
            past = hist[pl.ds(pl.multiple_of(g * GROUP * STATE, GROUP * STATE), GROUP * STATE), :]
            local = jnp.dot(cblk[span, :], past, preferred_element_type=jnp.float32)
            out[span, cols] = local + skip_w[:, cols] * mixed[span, cols].astype(jnp.float32)

        def group(g, state):
            emit(jnp.maximum(g - 1, 0))
            at = pl.multiple_of(g * GROUP, GROUP)
            step_blk = steps[pl.ds(at, GROUP), cols]
            drive_blk = drive[pl.ds(at, GROUP), cols]
            for i in range(GROUP):
                b_row = jnp.concatenate([bwide[at + i]] * (tile // 128), axis=1)
                state = jnp.exp2(step_blk[i:i + 1] * decay) * state + b_row * drive_blk[i:i + 1]
                hist[pl.ds(pl.multiple_of((at + i) * STATE, STATE), STATE), :] = state.astype(jnp.bfloat16)
            return state

        ends[:, cols] = lax.fori_loop(0, groups, group, jnp.zeros((STATE, tile), jnp.float32))
        emit(groups - 1)


def fix_kernel(local, summed, cblk, incoming, rates, out, hist):
    rows, width = local.shape
    tile = tile_of(width)
    groups = rows // GROUP

    @pl.loop(0, width // tile)
    def _(c):
        cols = pl.ds(pl.multiple_of(c * tile, tile), tile)
        decay = rates[:, cols] * (-LOG2E)
        start = incoming[:, cols]

        def emit(g):
            span = pl.ds(pl.multiple_of(g * GROUP, GROUP), GROUP)
            past = hist[pl.ds(pl.multiple_of(g * GROUP * STATE, GROUP * STATE), GROUP * STATE), :]
            fixed = jnp.dot(cblk[span, :], past, preferred_element_type=jnp.float32)
            out[span, cols] = (local[span, cols] + fixed).astype(out.dtype)

        @pl.loop(0, groups)
        def _(g):
            emit(jnp.maximum(g - 1, 0))
            at = pl.multiple_of(g * GROUP, GROUP)
            sum_blk = summed[pl.ds(at, GROUP), cols]
            for i in range(GROUP):
                moved = jnp.exp2(sum_blk[i:i + 1] * decay) * start
                hist[pl.ds(pl.multiple_of((at + i) * STATE, STATE), STATE), :] = moved.astype(jnp.bfloat16)

        emit(groups - 1)


def layer(current, before, gain, conv_w, conv_b, x_w, dt_w, dt_b, rates, skip_w):
    rows, width = current.shape
    tile = tile_of(width)
    f32, bf16 = jnp.float32, jnp.bfloat16
    local, ends, summed, cblk = pl.pallas_call(
        scan_kernel,
        out_shape=(
            jax.ShapeDtypeStruct((rows, width), f32),
            jax.ShapeDtypeStruct((STATE, width), f32),
            jax.ShapeDtypeStruct((rows, width), f32),
            jax.ShapeDtypeStruct((rows, GROUP * STATE), bf16),
        ),
        in_specs=[VMEM] * 10,
        out_specs=(VMEM,) * 4,
        scratch_shapes=[
            pltpu.VMEM((rows + PAD, width), f32),
            pltpu.VMEM((rows, width), bf16),
            pltpu.VMEM((rows, width), f32),
            pltpu.VMEM((rows, width), f32),
            pltpu.VMEM((rows, STATE, 128), f32),
            pltpu.VMEM((rows * STATE, tile), bf16),
        ],
        compiler_params=pltpu.CompilerParams(vmem_limit_bytes=40 << 20),
        name="local_scan",
    )(current, before, gain, conv_w, conv_b, x_w, dt_w, dt_b, rates, skip_w)
    incoming = relay_carries(summed[-1:], ends, rates)
    return pl.pallas_call(
        fix_kernel,
        out_shape=jax.ShapeDtypeStruct((rows, width), bf16),
        in_specs=[VMEM] * 5,
        out_specs=VMEM,
        scratch_shapes=[pltpu.VMEM((rows * STATE, tile), bf16)],
        compiler_params=pltpu.CompilerParams(vmem_limit_bytes=40 << 20),
        name="carry_fix",
    )(local, summed, cblk, incoming, rates)


def local(acts, feed, norm_gain, conv_weight, conv_bias, x_proj, dt_proj, dt_bias, a_rate, skip):
    section_zero = lax.axis_index("section") == 0
    seq_zero = lax.axis_index("seq") == 0
    weights = (norm_gain, conv_weight[0], conv_bias, x_proj[0], dt_proj[0], dt_bias, a_rate[0], skip)
    current = acts[0]
    tails = passed_along(jnp.concatenate([acts[:, -PAD:], feed[:, -PAD:]], 0), "seq", 1)
    prev_now, prev_feeds = (tails[0], tails[1:])
    results = []
    for tick in range(TICKS):
        result = layer(current, prev_now, *weights)
        results.append(result)
        if tick + 1 < TICKS:
            received = passed_along(result, "section", 1)
            current = jnp.where(section_zero, feed[tick], received)
            diagonal = passed_along(result[-PAD:], ("section", "seq"), lax.axis_size("seq") + 1)
            diagonal = jnp.where(seq_zero, jnp.zeros_like(diagonal), diagonal)
            prev_now = jnp.where(section_zero, prev_feeds[tick], diagonal)
    return jnp.stack(results, 0)[:, None]


def solution(mesh):
    return jax.shard_map(
        local,
        mesh=mesh,
        in_specs=(
            P("section", "seq", None),
            P(None, "seq", None),
            P("section", None),
            P("section", None, None),
            P("section", None),
            P("section", None, None),
            P("section", None, None),
            P("section", None),
            P("section", None, None),
            P("section", None),
        ),
        out_specs=P(None, "section", "seq", None),
        check_vma=False,
    )
```
